16 devices in a mesh: dp: 4 (over z, y), sp: 4 (over x, core).
Axes of the slice: x: 2, y: 2, z: 2, core: 2. Of those that a mesh axis runs over, the one named last changes fastest.
Arguments:
- hidden: bfloat16 [32, 768, 3072], P('dp', 'sp'), parts along dimension 0
- cond_vec: bfloat16 [32, 3072], P('dp'), parts along dimension 0
- pos_ids: int32 [768, 3], P('sp')
- w_mod: bfloat16 [2, 3072, 9216], replicated
- b_mod: bfloat16 [2, 9216], replicated
- w_in: bfloat16 [2, 3072, 21504], replicated
- b_in: bfloat16 [2, 21504], replicated
- q_gain: bfloat16 [2, 128], replicated
- k_gain: bfloat16 [2, 128], replicated
- w_out: bfloat16 [2, 15360, 3072], replicated
- b_out: bfloat16 [2, 3072], replicated
Outputs:
- output: bfloat16 [32, 768, 3072], P('dp', 'sp'), parts along dimension 0
There are 4 independent parts. The reference program is written for one: setup_inputs(seed, part) draws one part's arguments, and reference() takes and returns one part's arrays. A program takes and returns all parts, laid end to end along the dimension named above; an argument that names none is the same for every part.
All inputs are finite; a program needn't handle non-finite values.
Results may differ from the reference program's by a relative error of at most 0.0115895.
Values are sent between devices in bfloat16 or wider.
A program may use at most 2.25 GiB of HBM per device.

```python
import math
import jax
import jax.numpy as jnp
from jax import lax

BATCH = 8
TEXT_LEN = 256
IMG_LEN = 512
D = 3072
HEADS = 24
HEAD = 128
MLP_DIM = 12288
BLOCKS = 2
QUERY_ROWS = 256

SEQ_LEN = TEXT_LEN + IMG_LEN
ROPE_SPLIT = (16, 56, 56)
ROPE_THETA = 10000.0
NORM_EPS = 1e-6


def image_ids(rng_key):
    half_log = int(math.log2(IMG_LEN)) // 2
    widths = jnp.array([2 ** (half_log - 1), 2 ** half_log, 2 ** (half_log + 1)], dtype=jnp.int32)
    k_width, k_row, k_col = jax.random.split(rng_key, 3)
    grid_width = widths[jax.random.randint(k_width, (), 0, 3)]
    row_off = jax.random.randint(k_row, (), 0, 64)
    col_off = jax.random.randint(k_col, (), 0, 64)
    img_index = jnp.arange(IMG_LEN, dtype=jnp.int32)
    img_ids = jnp.stack([jnp.zeros_like(img_index), row_off + img_index // grid_width, col_off + img_index % grid_width], axis=1)
    return jnp.concatenate([jnp.zeros((TEXT_LEN, 3), jnp.int32), img_ids.astype(jnp.int32)], axis=0)


def setup_inputs(seed: int = 0, part: int = 0) -> dict:
    shared = jax.random.split(jax.random.key(seed), 9)
    part_key = jax.random.fold_in(jax.random.key(seed + 1), part)
    k_text, k_img, k_mean, k_cond = jax.random.split(part_key, 4)
    text_mean = jax.random.normal(k_mean, (D,), jnp.float32)
    text_rows = 0.6 * jax.random.normal(k_text, (BATCH, TEXT_LEN, D), jnp.float32) + text_mean
    img_rows = jax.random.normal(k_img, (BATCH, IMG_LEN, D), jnp.float32)
    hidden = jnp.concatenate([text_rows, img_rows], axis=1).astype(jnp.bfloat16)
    cond_vec = jax.random.normal(k_cond, (BATCH, D), jnp.float32).astype(jnp.bfloat16)
    pos_ids = image_ids(shared[0])
    w_mod = (jax.random.normal(shared[1], (BLOCKS, D, 3 * D), jnp.float32) * D ** -0.5).astype(jnp.bfloat16)
    b_mod = (0.3 * jax.random.normal(shared[2], (BLOCKS, 3 * D), jnp.float32)).astype(jnp.bfloat16)
    w_in = (jax.random.normal(shared[3], (BLOCKS, D, 3 * D + MLP_DIM), jnp.float32) * D ** -0.5).astype(jnp.bfloat16)
    b_in = (0.3 * jax.random.normal(shared[4], (BLOCKS, 3 * D + MLP_DIM), jnp.float32)).astype(jnp.bfloat16)
    q_gain = jax.random.uniform(shared[5], (BLOCKS, HEAD), jnp.float32, 0.8, 2.2).astype(jnp.bfloat16)
    k_gain = jax.random.uniform(shared[6], (BLOCKS, HEAD), jnp.float32, 0.8, 2.2).astype(jnp.bfloat16)
    w_out = (jax.random.normal(shared[7], (BLOCKS, D + MLP_DIM, D), jnp.float32) * (D + MLP_DIM) ** -0.5).astype(jnp.bfloat16)
    b_out = (0.3 * jax.random.normal(shared[8], (BLOCKS, D), jnp.float32)).astype(jnp.bfloat16)
    return dict(hidden=hidden, cond_vec=cond_vec, pos_ids=pos_ids, w_mod=w_mod, b_mod=b_mod, w_in=w_in, b_in=b_in, q_gain=q_gain, k_gain=k_gain, w_out=w_out, b_out=b_out)


def rope_tables(pos_ids):
    angle_parts = []
    for column, rope_dim in enumerate(ROPE_SPLIT):
        inv_freq = 1.0 / (ROPE_THETA ** (jnp.arange(0, rope_dim, 2, dtype=jnp.float32) / rope_dim))
        angle_parts.append(pos_ids[:, column:column + 1].astype(jnp.float32) * inv_freq)
    angles = jnp.concatenate(angle_parts, axis=1)
    return jnp.cos(angles), jnp.sin(angles)


def rms_norm(tensor, gain):
    sq_mean = jnp.mean(tensor * tensor, axis=-1, keepdims=True)
    return tensor * lax.rsqrt(sq_mean + NORM_EPS) * gain.astype(jnp.float32)


def apply_rope(tensor, cos_t, sin_t):
    paired = tensor.reshape(tensor.shape[:-1] + (tensor.shape[-1] // 2, 2))
    even_v = paired[..., 0]
    odd_v = paired[..., 1]
    cos_b = cos_t[:, None, :]
    sin_b = sin_t[:, None, :]
    rotated = jnp.stack([even_v * cos_b - odd_v * sin_b, even_v * sin_b + odd_v * cos_b], axis=-1)
    return rotated.reshape(tensor.shape)


def attention(queries, keys_all, values_all):
    key_f = keys_all.astype(jnp.float32)
    val_f = values_all.astype(jnp.float32)
    q_blocks = queries.reshape(SEQ_LEN // QUERY_ROWS, QUERY_ROWS, HEADS, HEAD)

    def one_block(q_blk):
        scores = jnp.einsum('qhd,khd->hqk', q_blk.astype(jnp.float32), key_f) * HEAD ** -0.5
        probs = jax.nn.softmax(scores, axis=-1)
        return jnp.einsum('hqk,khd->qhd', probs, val_f)

    return lax.map(one_block, q_blocks).reshape(SEQ_LEN, HEADS, HEAD).astype(jnp.bfloat16)


def single_block(hidden, cond_row, cos_t, sin_t, params):
    w_mod, b_mod, w_in, b_in, q_gain, k_gain, w_out, b_out = params
    mod_act = jax.nn.silu(cond_row.astype(jnp.float32)).astype(jnp.bfloat16)
    mod_vals = jnp.dot(mod_act[None, :], w_mod, preferred_element_type=jnp.float32)[0] + b_mod.astype(jnp.float32)
    mod_vals = mod_vals.astype(jnp.bfloat16).astype(jnp.float32)
    mod_shift = mod_vals[:D]
    mod_scale = mod_vals[D:2 * D]
    mod_gate = mod_vals[2 * D:]
    x_float = hidden.astype(jnp.float32)
    centered = x_float - jnp.mean(x_float, axis=-1, keepdims=True)
    normed = centered * lax.rsqrt(jnp.mean(centered * centered, axis=-1, keepdims=True) + NORM_EPS)
    modded = ((1.0 + mod_scale) * normed + mod_shift).astype(jnp.bfloat16)
    proj_in = (jnp.dot(modded, w_in, preferred_element_type=jnp.float32) + b_in.astype(jnp.float32)).astype(jnp.bfloat16)
    q_raw = proj_in[:, :D].reshape(SEQ_LEN, HEADS, HEAD).astype(jnp.float32)
    k_raw = proj_in[:, D:2 * D].reshape(SEQ_LEN, HEADS, HEAD).astype(jnp.float32)
    v_heads = proj_in[:, 2 * D:3 * D].reshape(SEQ_LEN, HEADS, HEAD)
    q_heads = apply_rope(rms_norm(q_raw, q_gain), cos_t, sin_t).astype(jnp.bfloat16)
    k_heads = apply_rope(rms_norm(k_raw, k_gain), cos_t, sin_t).astype(jnp.bfloat16)
    attn_out = attention(q_heads, k_heads, v_heads).reshape(SEQ_LEN, D)
    mlp_act = jax.nn.gelu(proj_in[:, 3 * D:].astype(jnp.float32), approximate=True).astype(jnp.bfloat16)
    joined = jnp.concatenate([attn_out, mlp_act], axis=1)
    block_out = (jnp.dot(joined, w_out, preferred_element_type=jnp.float32) + b_out.astype(jnp.float32)).astype(jnp.bfloat16)
    return (x_float + mod_gate * block_out.astype(jnp.float32)).astype(jnp.bfloat16)


def reference(hidden, cond_vec, pos_ids, w_mod, b_mod, w_in, b_in, q_gain, k_gain, w_out, b_out):
    cos_t, sin_t = rope_tables(pos_ids)
    stacked = (w_mod, b_mod, w_in, b_in, q_gain, k_gain, w_out, b_out)

    def one_item(item_pair):
        tokens, cond_row = item_pair

        def layer_step(state, params):
            return single_block(state, cond_row, cos_t, sin_t, params), None

        final_x, _ = lax.scan(layer_step, tokens, stacked)
        return final_x

    return lax.map(one_item, (hidden, cond_vec))
```

```python
import functools
import math
import jax
import jax.numpy as jnp
from jax import lax
from jax.experimental import pallas as pl
from jax.experimental.pallas import tpu as pltpu
from jax.sharding import PartitionSpec as P

HEAD = 128
HEADS = 24
D = 3072
MLP = 12288
QKV = 3 * D
NIN = QKV + MLP
ROWS = 192
ITEMS = 2
BLK = ITEMS * ROWS
HALF = 2 * BLK
GROUP = 4
LAYERS = 2
ROPE_SPLIT = (16, 56, 56)
ROPE_THETA = 10000.0
EPS = 1e-6
GELU_C = math.sqrt(2.0 / math.pi)
VMEM_LIMIT = 62 * 1024 * 1024
bf16 = jnp.bfloat16
f32 = jnp.float32


def dot(a, b):
    return jnp.dot(a, b, preferred_element_type=f32)


def layer_row(ref, layer, cs):
    both = ref[:, cs].astype(f32)
    return jnp.where(layer == 0, both[0:1], both[1:2])


def mod_cols(mod_ref, item, lo, hi):
    q = QKV // GROUP
    parts = []
    while lo < hi:
        end = min(hi, (lo // q + 1) * q)
        parts.append(mod_ref[lo // q, item:item + 1, lo % q:lo % q + end - lo])
        lo = end
    return parts[0] if len(parts) == 1 else jnp.concatenate(parts, axis=1)


def mod_body(s_ref, c_ref, w_ref, b_ref, o_ref):
    act = jax.nn.silu(c_ref[...].astype(f32)).astype(bf16)
    bias = layer_row(b_ref, pl.program_id(0), slice(None))
    o_ref[...] = (dot(act, w_ref[...]) + bias).astype(bf16)


def modulation(me, cond, w_mod, b_mod, tn=768):
    items = cond.shape[0]
    per = QKV // GROUP // tn
    return pl.pallas_call(
        mod_body,
        grid_spec=pltpu.PrefetchScalarGridSpec(
            num_scalar_prefetch=1,
            grid=(LAYERS, per),
            in_specs=[
                pl.BlockSpec((items, D), lambda l, n, s: (0, 0)),
                pl.BlockSpec((None, D, tn), lambda l, n, s: (l, 0, s[0] * per + n)),
                pl.BlockSpec((LAYERS, tn), lambda l, n, s: (0, s[0] * per + n)),
            ],
            out_specs=pl.BlockSpec((None, items, tn), lambda l, n, s: (l, 0, n)),
        ),
        out_shape=jax.ShapeDtypeStruct((LAYERS, items, QKV // GROUP), bf16),
        compiler_params=pltpu.CompilerParams(dimension_semantics=("arbitrary", "arbitrary"), vmem_limit_bytes=VMEM_LIMIT),
        cost_estimate=pl.CostEstimate(flops=2 * 16 * D * QKV // 2, bytes_accessed=D * QKV, transcendentals=items * D),
        name="modulation",
    )(me, cond, w_mod, b_mod)


def norm_rows(x_ref, u_ref, mod8_ref, base, ubase, sub, lc):
    def step(i, carry):
        r = pl.ds(pl.multiple_of(base + i * sub, sub), sub)
        ru = pl.ds(pl.multiple_of(ubase + i * sub, sub), sub)
        tot = jnp.zeros((sub, HEAD), f32)
        for c in range(D // lc):
            x = x_ref[r, c * lc:(c + 1) * lc].astype(f32)
            for j in range(lc // HEAD):
                tot += x[:, j * HEAD:(j + 1) * HEAD]
        mu = jnp.sum(tot, axis=-1, keepdims=True) * (1.0 / D)
        tot = jnp.zeros((sub, HEAD), f32)
        for c in range(D // lc):
            x = x_ref[r, c * lc:(c + 1) * lc].astype(f32)
            for j in range(lc // HEAD):
                d = x[:, j * HEAD:(j + 1) * HEAD] - mu
                tot += d * d
        rs = lax.rsqrt(jnp.sum(tot, axis=-1, keepdims=True) * (1.0 / D) + EPS)
        for c in range(D // lc):
            cs = slice(c * lc, (c + 1) * lc)
            x = x_ref[r, cs].astype(f32)
            xn = ((x - mu) * rs).reshape(sub // 8, 8, lc)
            y = xn * mod8_ref[1][None, :, cs] + mod8_ref[0][None, :, cs]
            u_ref[ru, cs] = y.reshape(sub, lc).astype(bf16)
        return carry

    lax.fori_loop(0, ROWS // sub, step, 0)


def swap_pairs(t):
    even = lax.broadcasted_iota(jnp.int32, t.shape, 1) % 2 == 0
    return jnp.where(even, pltpu.roll(t, HEAD - 1, 1), pltpu.roll(t, 1, 1))


def in_body(s_ref, x0_ref, x1_ref, mod_ref, w_ref, b_ref, t0_ref, t1_ref, qg_ref, kg_ref, *refs, tn, cw, n_after):
    qkv_ref, g_ref, u_ref, h_ref, mod8_ref, tab_ref = refs[n_after:]
    n = pl.program_id(0)
    nq = D // tn
    nt = NIN // tn

    @pl.when(n == 0)
    def _():
        for i, gain_ref in enumerate((qg_ref, kg_ref)):
            gain = jnp.broadcast_to(layer_row(gain_ref, s_ref[0], slice(None)), (8, HEAD))
            swapped = swap_pairs(gain)
            for blk, t_ref in enumerate((t0_ref, t1_ref)):
                for j, g in enumerate((gain, swapped)):
                    t = t_ref[j].reshape(ROWS // 8, 8, HEAD) * g[None]
                    tab_ref[i, j, blk * ROWS:(blk + 1) * ROWS] = t.reshape(ROWS, HEAD)
        for it in range(ITEMS):
            mod8_ref[0] = jnp.broadcast_to(mod_cols(mod_ref, it, 0, D).astype(f32), (8, D))
            mod8_ref[1] = jnp.broadcast_to(1.0 + mod_cols(mod_ref, it, D, 2 * D).astype(f32), (8, D))
            for blk, x_ref in enumerate((x0_ref, x1_ref)):
                norm_rows(x_ref, u_ref, mod8_ref, it * ROWS, (2 * blk + it) * ROWS, 96, 256)

    def mm(c):
        cs = slice(c * cw, (c + 1) * cw)
        acc = dot(u_ref[...], w_ref[:, cs]) + layer_row(b_ref, s_ref[0], cs)
        h_ref[:, cs] = acc.astype(bf16)

    def qk_post(c):
        i = jnp.clip((n - 1) // nq, 0, 1)
        tab = [
            jnp.concatenate([tab_ref[i, j, blk * ROWS:(blk + 1) * ROWS] for blk in (0, 0, 1, 1)], axis=0) for j in range(2)
        ]
        for hd in range(cw // HEAD):
            hs = slice(c * cw + hd * HEAD, c * cw + (hd + 1) * HEAD)
            hh = h_ref[:, hs].astype(f32)
            r = lax.rsqrt(jnp.sum(hh * hh, axis=-1, keepdims=True) * (1.0 / HEAD) + EPS)
            qkv_ref[:, hs] = ((hh * tab[0] + swap_pairs(hh) * tab[1]) * r).astype(bf16)

    def v_post(c):
        cs = slice(c * cw, (c + 1) * cw)
        qkv_ref[:, cs] = h_ref[:, cs]

    def g_post(c):
        cs = slice(c * cw, (c + 1) * cw)
        h = h_ref[:, cs].astype(f32)
        t = jnp.tanh(h * (GELU_C + (GELU_C * 0.044715) * (h * h)))
        hf = 0.5 * h
        g_ref[:, cs] = (hf + hf * t).astype(bf16)

    nc = tn // cw

    @pl.when(n <= 2 * nq)
    def _():
        for c in range(nc):
            qk_post(c)
            mm(c)

    @pl.when(jnp.logical_and(n > 2 * nq, n <= 3 * nq))
    def _():
        for c in range(nc):
            v_post(c)
            mm(c)

    @pl.when(jnp.logical_and(n > 3 * nq, n < nt))
    def _():
        for c in range(nc):
            g_post(c)
            mm(c)

    @pl.when(n == nt)
    def _():
        for c in range(nc):
            g_post(c)


def project_in(scalars, x0, x1, mod, w_in, b_in, tab, q_gain, k_gain, after, tn=1024, cw=256):
    nq = D // tn
    nt = NIN // tn
    one = pl.Buffered(1)
    cur = lambda n: jnp.minimum(n, nt - 1)
    prev = lambda n: jnp.maximum(n - 1, 0)
    return pl.pallas_call(
        functools.partial(in_body, tn=tn, cw=cw, n_after=len(after)),
        grid_spec=pltpu.PrefetchScalarGridSpec(
            num_scalar_prefetch=1,
            grid=(nt + 1,),
            in_specs=[
                pl.BlockSpec((BLK, D), lambda n, l: (0, 0), pipeline_mode=one),
                pl.BlockSpec((BLK, D), lambda n, l: (0, 0), pipeline_mode=one),
                pl.BlockSpec((None, GROUP, ITEMS, QKV // GROUP), lambda n, s: (s[0], 0, 0, 0), pipeline_mode=one),
                pl.BlockSpec((None, D, tn), lambda n, s: (s[0], 0, cur(n))),
                pl.BlockSpec((LAYERS, tn), lambda n, s: (0, cur(n))),
                pl.BlockSpec((2, None, ROWS, HEAD), lambda n, s: (0, s[1], 0, 0), pipeline_mode=one),
                pl.BlockSpec((2, None, ROWS, HEAD), lambda n, s: (0, s[2], 0, 0), pipeline_mode=one),
                pl.BlockSpec((LAYERS, HEAD), lambda n, s: (0, 0), pipeline_mode=one),
                pl.BlockSpec((LAYERS, HEAD), lambda n, s: (0, 0), pipeline_mode=one),
            ] + [pl.BlockSpec(memory_space=pl.ANY)] * len(after),
            out_specs=[
                pl.BlockSpec((HALF, tn), lambda n, l: (0, jnp.minimum(prev(n), 3 * nq - 1))),
                pl.BlockSpec((HALF, tn), lambda n, l: (0, jnp.maximum(prev(n) - 3 * nq, 0))),
            ],
            scratch_shapes=[
                pltpu.VMEM((HALF, D), bf16),
                pltpu.VMEM((HALF, tn), bf16),
                pltpu.VMEM((2, 8, D), f32),
                pltpu.VMEM((2, 2, BLK, HEAD), f32),
            ],
        ),
        out_shape=[jax.ShapeDtypeStruct((HALF, QKV), bf16), jax.ShapeDtypeStruct((HALF, MLP), bf16)],
        compiler_params=pltpu.CompilerParams(dimension_semantics=("arbitrary",), vmem_limit_bytes=VMEM_LIMIT),
        cost_estimate=pl.CostEstimate(
            flops=2 * HALF * D * NIN, bytes_accessed=2 * D * NIN + 2 * HALF * (NIN + D), transcendentals=HALF * MLP
        ),
        name="project_in",
    )(scalars, x0, x1, mod, w_in, b_in, tab, tab, q_gain, k_gain, *after)


def attn_body(*refs, nq, nh, qw):
    q_refs = refs[:nq]
    k_refs = refs[nq:nq + 2]
    v_refs = refs[nq + 2:nq + 4]
    o_refs = refs[nq + 4:2 * nq + 4]
    s_refs = refs[2 * nq + 4:]
    to_exp2 = HEAD ** -0.5 * math.log2(math.e)
    nqr = nq * 2 * ROWS
    nk = GROUP * ROWS
    kq = {}
    outs = {h: [] for h in range(nh)}

    def rows(rs, hs):
        return jnp.concatenate([r[b, :, hs] for r in rs for b in range(2)], axis=0)

    def load(h):
        hs = slice(h * HEAD, (h + 1) * HEAD)
        kq[h] = (rows(k_refs, hs), rows(q_refs, hs), rows(v_refs, hs).T)

    def front(h, a, slot):
        if h not in kq:
            load(h)
        k, q, _ = kq[h]
        m = None
        for j in range(0, nk, 256):
            s = lax.dot_general(k[j:j + 256], q[a:a + qw], (((1,), (1,)), ((), ())), preferred_element_type=f32)
            s_refs[slot][j:j + 256] = s
            mj = jnp.max(s.reshape(32, 8, qw), axis=0)
            m = mj if m is None else jnp.maximum(m, mj)
        return jnp.max(m, axis=0, keepdims=True)

    def back(h, a, slot, m):
        vt = kq[h][2]
        mc = jnp.broadcast_to(m * to_exp2, (8, qw))
        l = None
        ot = None
        for j in range(0, nk, 256):
            s = s_refs[slot][j:j + 256].reshape(32, 8, qw)
            p = jnp.exp2(s * to_exp2 - mc[None])
            lj = jnp.sum(p, axis=0)
            l = lj if l is None else l + lj
            oj = dot(vt[:, j:j + 256], p.reshape(256, qw).astype(bf16))
            ot = oj if ot is None else ot + oj
        l = jnp.sum(l, axis=0, keepdims=True)
        outs[h].append((ot * (1.0 / l)).T.astype(bf16))
        if a + qw >= nqr:
            o = jnp.concatenate(outs[h], axis=0)
            for j in range(nqr // ROWS):
                o_refs[j // 2][j % 2, :, h * HEAD:(h + 1) * HEAD] = o[j * ROWS:(j + 1) * ROWS]

    prev = None
    chunks = [(h, a) for h in range(nh) for a in range(0, nqr, qw)]
    for i, chunk in enumerate(chunks + [None]):
        this = None
        if chunk is not None:
            this = (*chunk, i % 2, front(*chunk, i % 2))
        if prev is not None:
            back(*prev)
        prev = this


def attention(qkvs, nh=12, qw=256):
    nq = len(qkvs)
    ng = HEADS // nh
    spec = lambda off: pl.BlockSpec((2, None, ROWS, nh * HEAD), lambda i, h: (0, i, 0, off * ng + h))
    views = [a.reshape(2, ITEMS, ROWS, QKV) for a in qkvs]
    pairs = ITEMS * HEADS * nq * 2 * ROWS * GROUP * ROWS
    outs = pl.pallas_call(
        functools.partial(attn_body, nq=nq, nh=nh, qw=qw),
        grid=(ITEMS, ng),
        in_specs=[spec(0)] * nq + [spec(1)] * 2 + [spec(2)] * 2,
        out_specs=[spec(0)] * nq,
        scratch_shapes=[pltpu.VMEM((GROUP * ROWS, qw), f32)] * 2,
        out_shape=[jax.ShapeDtypeStruct((2, ITEMS, ROWS, D), bf16)] * nq,
        compiler_params=pltpu.CompilerParams(dimension_semantics=("arbitrary", "arbitrary"), vmem_limit_bytes=VMEM_LIMIT),
        cost_estimate=pl.CostEstimate(flops=4 * pairs * HEAD, bytes_accessed=2 * 8 * HALF * D, transcendentals=pairs),
        name="attention",
    )(*views, *views, *views)
    return [o.reshape(HALF, D) for o in outs]


def out_body(s_ref, *refs, nb, tk, cw):
    o_ref, g_ref, w_ref, b_ref, mod_ref = refs[:5]
    x_refs = refs[5:5 + nb]
    y_refs = refs[5 + nb:5 + 2 * nb]
    acc_ref, x_buf, y_buf, isem, osem = refs[5 + 2 * nb:]
    k = pl.program_id(0)
    no = D // tk
    nk = (D + MLP) // tk

    def x_copy(b):
        return pltpu.make_async_copy(x_refs[b], x_buf.at[pl.ds(b * BLK, BLK)], isem.at[b])

    def cols(c):
        return slice(c * cw, (c + 1) * cw)

    @pl.when(k == 0)
    def _():
        for b in range(nb):
            x_copy(b).start()
        for c in range(D // cw):
            acc_ref[:, cols(c)] = dot(o_ref[...], w_ref[:, cols(c)])

    @pl.when(jnp.logical_and(k > 0, k < no))
    def _():
        for c in range(D // cw):
            acc_ref[:, cols(c)] += dot(o_ref[...], w_ref[:, cols(c)])

    @pl.when(jnp.logical_and(k >= no, k < nk - 1))
    def _():
        for c in range(D // cw):
            acc_ref[:, cols(c)] += dot(g_ref[...], w_ref[:, cols(c)])

    @pl.when(k == nk - 1)
    def _():
        for b in range(nb):
            x_copy(b).wait()
        for c in range(D // cw):
            cs = cols(c)
            y = acc_ref[:, cs] + dot(g_ref[...], w_ref[:, cs])
            y = (y + layer_row(b_ref, s_ref[0], cs)).astype(bf16).astype(f32)
            for b in range(nb):
                for it in range(ITEMS):
                    rs = slice(b * BLK + it * ROWS, b * BLK + (it + 1) * ROWS)
                    gate = mod_cols(mod_ref, it, 2 * D + c * cw, 2 * D + (c + 1) * cw).astype(f32)
                    y_buf[rs, cs] = (x_buf[rs, cs].astype(f32) + gate * y[rs]).astype(bf16)
            for b in range(nb):
                pltpu.make_async_copy(
                    y_buf.at[pl.ds(b * BLK, BLK), pl.ds(c * cw, cw)], y_refs[b].at[:, pl.ds(c * cw, cw)], osem.at[b]
                ).start()
        for b in range(nb):
            pltpu.make_async_copy(y_buf.at[pl.ds(b * BLK, BLK)], y_refs[b], osem.at[b]).wait()


def project_out(layer, o, g, w_out, b_out, mod, xs, rb, tk=1024, cw=512):
    nb = len(xs)
    r = BLK * nb
    no = D // tk
    nk = (D + MLP) // tk
    one = pl.Buffered(1)
    hbm = pl.BlockSpec(memory_space=pl.ANY)
    return pl.pallas_call(
        functools.partial(out_body, nb=nb, tk=tk, cw=cw),
        grid_spec=pltpu.PrefetchScalarGridSpec(
            num_scalar_prefetch=1,
            grid=(nk,),
            in_specs=[
                pl.BlockSpec((r, tk), lambda k, l: (l[1], jnp.minimum(k, no - 1))),
                pl.BlockSpec((r, tk), lambda k, l: (l[1], jnp.maximum(k - no, 0))),
                pl.BlockSpec((None, tk, D), lambda k, l: (l[0], k, 0)),
                pl.BlockSpec((LAYERS, D), lambda k, l: (0, 0), pipeline_mode=one),
                pl.BlockSpec((None, GROUP, ITEMS, QKV // GROUP), lambda k, l: (l[0], 0, 0, 0), pipeline_mode=one),
            ] + [hbm] * nb,
            out_specs=[hbm] * nb,
            scratch_shapes=[
                pltpu.VMEM((r, D), f32),
                pltpu.VMEM((r, D), bf16),
                pltpu.VMEM((r, D), bf16),
                pltpu.SemaphoreType.DMA((nb,)),
                pltpu.SemaphoreType.DMA((nb,)),
            ],
        ),
        out_shape=[jax.ShapeDtypeStruct((BLK, D), bf16)] * nb,
        compiler_params=pltpu.CompilerParams(dimension_semantics=("arbitrary",), vmem_limit_bytes=VMEM_LIMIT),
        cost_estimate=pl.CostEstimate(
            flops=2 * r * D * (D + MLP), bytes_accessed=2 * D * (D + MLP) + 2 * r * (3 * D + MLP), transcendentals=0
        ),
        name="project_out",
    )(jnp.array([layer, rb], jnp.int32), o, g, w_out, b_out, mod, *xs)


def place_body(s_ref, *refs):
    o_ref = refs[GROUP]
    for k in range(GROUP):
        @pl.when(pl.program_id(0) == k)
        def _(k=k):
            o_ref[...] = refs[k][...].reshape(o_ref.shape)


def place(me, blocks):
    return pl.pallas_call(
        place_body,
        grid_spec=pltpu.PrefetchScalarGridSpec(
            num_scalar_prefetch=1,
            grid=(GROUP,),
            in_specs=[pl.BlockSpec((BLK, D), lambda k, s: (0, 0), pipeline_mode=pl.Buffered(1))] * GROUP,
            out_specs=pl.BlockSpec((ITEMS, ROWS, D), lambda k, s: (jnp.bitwise_xor(s[0], k), 0, 0)),
        ),
        out_shape=jax.ShapeDtypeStruct((GROUP * ITEMS, ROWS, D), bf16),
        compiler_params=pltpu.CompilerParams(dimension_semantics=("arbitrary",), vmem_limit_bytes=VMEM_LIMIT),
        cost_estimate=pl.CostEstimate(flops=0, bytes_accessed=4 * GROUP * BLK * D, transcendentals=0),
        name="place",
    )(me, *blocks)


def rope_table(pos):
    lane = jnp.arange(HEAD, dtype=jnp.int32)
    pair = lane // 2
    ang = None
    start = 0
    for column, dim in enumerate(ROPE_SPLIT):
        freq = 1.0 / (ROPE_THETA ** ((2 * pair - start).astype(f32) / dim))
        part = pos[:, :, column:column + 1].astype(f32) * freq
        ang = part if ang is None else jnp.where(lane >= start, part, ang)
        start += dim
    return jnp.stack([jnp.cos(ang), jnp.where(lane % 2 == 0, -1.0, 1.0) * jnp.sin(ang)])


def solution(mesh):
    def local(hidden, cond, pos_ids, w_mod, b_mod, w_in, b_in, q_gain, k_gain, w_out, b_out):
        me = lax.axis_index("sp").astype(jnp.int32)
        me1 = me.reshape(1)
        source = [jnp.bitwise_xor(me, k) for k in range(GROUP)]
        swap = lambda a, k: lax.ppermute(a, "sp", [(i, i ^ k) for i in range(GROUP)])
        piece = lambda k: lax.dynamic_slice_in_dim(hidden, ITEMS * source[k], ITEMS, axis=0).reshape(BLK, D)

        x = [piece(0), swap(piece(1), 1)]
        tab = rope_table(lax.all_gather(pos_ids, "sp"))
        part = modulation(me1, cond, w_mod, b_mod).reshape(LAYERS, GROUP, ITEMS, QKV // GROUP)
        mod = lax.all_to_all(part, "sp", 1, 1)
        far = [piece(2), piece(3)]
        far, mod, x, tab = lax.optimization_barrier((far, mod, x, tab))
        x += [swap(far[0], 2), swap(far[1], 3)]

        for layer in range(LAYERS):
            halves = []
            for i in range(2):
                scalars = jnp.stack([jnp.int32(layer), source[2 * i], source[2 * i + 1]])
                after = [h[0] for h in halves] if halves else [x[0]]
                halves.append(
                    project_in(scalars, x[2 * i], x[2 * i + 1], mod, w_in, b_in, tab, q_gain, k_gain, [after[0]])
                )
            att = attention([h[0] for h in halves])
            if layer < LAYERS - 1:
                x = [
                    y
                    for i in range(2)
                    for y in project_out(layer, att[i], halves[i][1], w_out, b_out, mod, x[2 * i:2 * i + 2], 0)
                ]
        out = {}
        for k in (2, 3, 1, 0):
            i = k // 2
            out[k] = project_out(layer, att[i], halves[i][1], w_out, b_out, mod, [x[k]], k % 2, tk=1536)[0]
            if k:
                out[k] = swap(out[k], k)
        return place(me1, [out[k] for k in range(GROUP)])

    rows = P("dp", "sp", None)
    rep = P()
    specs = (rows, P("dp", None), P("sp", None)) + (rep,) * 8
    return jax.shard_map(local, mesh=mesh, in_specs=specs, out_specs=rows, check_vma=False)
```
